512 devices in a mesh: row: 8 (over x, z_hi), col: 16 (over y, core), layer: 4 (over z_lo).
Axes of the slice: x: 4, y: 8, z: 8 (z_hi: 2, z_lo: 4; z = z_hi * 4 + z_lo), core: 2. Of those that a mesh axis runs over, the one named last changes fastest.
Arguments:
- panel: float32 [1024, 8192], P('layer', ('col', 'row')), may hold values from -0.75 to 0.75
- c_in: float32 [16, 8, 64, 8192], P('layer', 'row', None, 'col'), may hold values from -1.5 to 1.5
Outputs:
- updated: float32 [16, 8, 64, 8192], P('layer', 'row', None, 'col')
The draws below stay inside these ranges and needn't reach their ends.
All inputs are finite; a program needn't handle non-finite values.
Results may differ from the reference program's by a relative error of at most 0.000062.
Values sent between devices are 32-bit elements; how exact they have to be, the bound alone decides.
A program may use at most 64 MiB of HBM per device.

```python
import jax
import jax.numpy as jnp
from jax import lax

N = 8192
K = 1024
W = 64
N_ROW = 8
N_COL = 16


def steps_of(stream_key, extent, pieces, smallest, largest):
    level = 1.0
    for position, parts in pieces:
        draws = jax.random.uniform(jax.random.fold_in(jax.random.fold_in(stream_key, 6), position), (parts,), jnp.float32, smallest / len(pieces), largest / len(pieces))
        level = level * jnp.repeat(jnp.exp(draws), extent[position] // parts).reshape((-1,) + (1,) * (len(extent) - 1 - position))
    return level


def noise(key, shape, spread, limit, shards=(), held_as=jnp.bfloat16):
    values = spread * jax.random.normal(key, shape, jnp.float32)
    if shards:
        values = values * steps_of(key, shape, shards, -0.22, 0.18)
    return jnp.clip(values, -limit, limit).astype(held_as)


def setup_inputs(seed: int = 0) -> dict:
    arg_keys = jax.random.split(jax.random.key(seed), 3)
    return {
        "panel": noise(arg_keys[0], (K, N), (0.3 * K ** -0.25), 0.75, ((0, 4), (1, 128)), jnp.float32),
        "c_in": noise(arg_keys[1], (N_COL, N_ROW, W, N), 0.1, 1.5, ((0, 4), (1, 8), (3, 16)), jnp.float32),
    }


def reference(panel, c_in):
    gram = lax.dot_general(panel, panel, (((0,), (0,)), ((), ())), precision=lax.Precision.HIGHEST, preferred_element_type=jnp.float32)
    gram = gram.reshape(N_COL, N_ROW, N // (N_ROW * N_COL), N)
    return c_in + gram
```

```python
import functools

import jax
import jax.numpy as jnp
from jax import lax
from jax.experimental import pallas as pl
from jax.experimental.pallas import tpu as pltpu
from jax.sharding import Mesh
from jax.sharding import PartitionSpec as P

NX, NY, NZ, NL = 4, 8, 8, 4
W, DEPTH = 64, 256
HALF = W // 2
C0 = 0
Y0 = 32
D0 = 35
Q0 = 39
P0 = 43
SLOTS = 51
RZ, RXP, RXM, RXA, RXB, RY, RD, RQA, RQB, RP, SEMS = 0, 8, 16, 24, 32, 40, 43, 47, 51, 55, 63


def kernel(panel_ref, out_ref, buf, left, send, recv, ready):
    x, zh, y = lax.axis_index("x"), lax.axis_index("zh"), lax.axis_index("y")
    core, zl = lax.axis_index("core"), lax.axis_index("zl")
    z = zh * NL + zl
    q = y % 2
    xp, xm = (x + 1) % NX, (x + NX - 1) % NX
    bar = pltpu.get_barrier_semaphore()

    def on_x(t):
        return {"x": t}

    def on_y(d):
        return {"y": (y + NY + d) % NY}

    def on_z(t):
        return {"zh": t // NL, "zl": t % NL}

    other = {"core": 1 - core}

    def signal(sem, where):
        pl.semaphore_signal(sem, inc=1, device_id=where, device_id_type=pl.DeviceIdType.MESH)

    for where in (on_x(xp), on_x(xm), on_y(1), on_y(-1), on_y(2), on_y(-2), on_y(4), other):
        signal(bar, where)
    for t in range(NZ):

        @pl.when(t > z)
        def _():
            signal(bar, on_z(t))

    def column_slot(i, t):
        return C0 + (t % NL) * 2 * NX + i * 2 + t // NL

    mine = column_slot(x, z)
    buf[mine] = panel_ref[...]

    pl.semaphore_wait(bar, 8 + z)
    for t in range(NZ):

        @pl.when(t < z)
        def _():
            signal(ready.at[z], on_z(t))

    def copy(src, dst, sem, where, part=None):
        a, b = buf.at[src], buf.at[dst]
        if part is not None:
            a, b = a.at[pl.ds(part * HALF, HALF)], b.at[pl.ds(part * HALF, HALF)]
        return pltpu.make_async_remote_copy(
            src_ref=a,
            dst_ref=b,
            send_sem=send.at[sem],
            recv_sem=recv.at[sem],
            device_id=where,
            device_id_type=pl.DeviceIdType.MESH,
        )

    def arrived(dst, sem, part=None):
        copy(dst, dst, sem, other, part).wait_recv()

    def z_copy(t):
        return pltpu.make_async_remote_copy(
            src_ref=panel_ref,
            dst_ref=buf.at[mine],
            send_sem=send.at[RZ + t],
            recv_sem=recv.at[RZ + z],
            device_id=on_z(t),
            device_id_type=pl.DeviceIdType.MESH,
        )

    def z_send(t):
        @pl.when(t > z)
        def _():
            pl.semaphore_wait(ready.at[t], 1)
            z_copy(t).start()

    def x_spread(t):
        slot = column_slot(x, t)
        copy(slot, slot, RXP + t, on_x(xp)).start()
        copy(slot, slot, RXM + t, on_x(xm)).start()

    def x_first(t):
        arrived(column_slot(x, t), RZ + t)
        x_spread(t)

    def x_second(t):
        slot = column_slot(xm, t)
        arrived(slot, RXP + t)
        copy(slot, slot, RXA + t, on_x(xp), 0).start()
        slot = column_slot(xp, t)
        arrived(slot, RXM + t)
        copy(slot, slot, RXB + t, on_x(xm), 1).start()

    def x_last(t):
        slot = column_slot((x + 2) % NX, t)
        arrived(slot, RXA + t, 0)
        arrived(slot, RXB + t, 1)

    def y_home(j):
        return ((y + NY - 2 * j) % NY) // 2

    def y_send():
        for j in (1, 2, 3):
            copy(mine, Y0 + j - 1, RY + j - 1, on_y(2 * j)).start()

    def d_copy(j, home):
        return pltpu.make_async_remote_copy(
            src_ref=buf.at[Y0 + j - 1],
            dst_ref=buf.at[D0 + zl],
            send_sem=send.at[RD + j - 1],
            recv_sem=recv.at[RD + zl],
            device_id=on_z(zh * NL + home),
            device_id_type=pl.DeviceIdType.MESH,
        )

    def y_forward():
        for j in (1, 2, 3):
            arrived(Y0 + j - 1, RY + j - 1)
            home = y_home(j)

            @pl.when(home != zl)
            def _():
                d_copy(j, home).start()

    back = ((y + NY - 2 * zl - q) % NY) // 2
    at_home = back == 0

    def row_slot(layer):
        away = jnp.where(zl == layer, Y0 + back - 1, D0 + layer)
        return jnp.where(at_home, column_slot(x, zh * NL + layer), away)

    def d_forward(layer):
        @pl.when(jnp.logical_and(back != 0, zl != layer))
        def _():
            arrived(D0 + layer, RD + layer)

        slot = row_slot(layer)
        copy(slot, Q0 + layer, RQA + layer, on_y(1), 0).start()
        copy(slot, Q0 + layer, RQB + layer, on_y(-1), 1).start()
        p_copy(slot, q, layer).start()

    def p_copy(slot, parity, layer):
        return copy(slot, P0 + parity * NL + layer, RP + parity * NL + layer, other)

    def q_forward(layer):
        arrived(Q0 + layer, RQA + layer, 0)
        arrived(Q0 + layer, RQB + layer, 1)
        p_copy(Q0 + layer, 1 - q, layer).start()

    for t in range(NZ):

        @pl.when(t < z)
        def _():
            z_copy(t).start()

    x_spread(z)
    y_send()
    near = [(zl + k) % NL for k in (1, 2, 3)]

    @pl.when(zh == 0)
    def _():
        for t in near:
            z_send(t)
        x_second(z)
        for t in near:
            x_first(t)
        y_forward()
        for t in near:
            x_second(t)
        for layer in range(NL):
            d_forward(layer)
        for t in range(NL, NZ):
            z_send(t)
        for t in range(NL, NZ):
            x_first(t)
        for layer in range(NL):
            q_forward(layer)
        for t in range(NL, NZ):
            x_second(t)

    @pl.when(zh == 1)
    def _():
        for t in near:
            z_send(NL + t)
        for t in range(NL):
            x_first(t)
        x_second(z)
        for t in near:
            x_first(NL + t)
        y_forward()
        for t in range(NL):
            x_second(t)
        for layer in range(NL):
            d_forward(layer)
        for t in near:
            x_second(NL + t)
        for layer in range(NL):
            q_forward(layer)

    for parity in (0, 1):
        for layer in range(NL):
            arrived(P0 + parity * NL + layer, RP + parity * NL + layer)
    for t in range(NZ):
        x_last(t)

    for layer in range(NL):
        for parity in (0, 1):
            own = jnp.where(q == parity, row_slot(layer), Q0 + layer)
            theirs = P0 + parity * NL + layer
            a = buf[jnp.where(core == 0, own, theirs)]
            b = buf[jnp.where(core == 0, theirs, own)]
            left[pl.ds(parity * 2 * W, W), :] = a
            left[pl.ds(parity * 2 * W + W, W), :] = b
        right = buf[pl.ds(C0 + layer * 2 * NX, 2 * NX)].reshape(2 * NX * W, DEPTH)
        part = lax.dot_general(
            left[...],
            right,
            (((1,), (1,)), ((), ())),
            precision=lax.Precision.HIGHEST,
            preferred_element_type=jnp.float32,
        )
        if layer == 0:
            out_ref[...] = part
        else:
            out_ref[...] += part

    def sent(src, sem, part=None):
        copy(src, src, sem, other, part).wait_send()

    for t in range(NZ):

        @pl.when(t != z)
        def _():
            sent(mine, RZ + t)

        sent(mine, RXP + t)
        sent(mine, RXM + t)
        sent(mine, RXA + t, 0)
        sent(mine, RXB + t, 1)
    for j in (1, 2, 3):
        sent(mine, RY + j - 1)

        @pl.when(y_home(j) != zl)
        def _():
            sent(mine, RD + j - 1)

    for layer in range(NL):
        sent(mine, RQA + layer, 0)
        sent(mine, RQB + layer, 1)
        for parity in (0, 1):
            sent(mine, RP + parity * NL + layer)


def on_device(panel, c_in):
    gram = pl.pallas_call(
        kernel,
        out_shape=jax.ShapeDtypeStruct((256, 512), jnp.float32),
        in_specs=[pl.BlockSpec(memory_space=pltpu.VMEM)],
        out_specs=pl.BlockSpec(memory_space=pltpu.VMEM),
        scratch_shapes=[
            pltpu.VMEM((SLOTS, W, DEPTH), jnp.float32),
            pltpu.VMEM((4 * W, DEPTH), jnp.float32),
            pltpu.SemaphoreType.DMA((SEMS,)),
            pltpu.SemaphoreType.DMA((SEMS,)),
            pltpu.SemaphoreType.REGULAR((NZ,)),
        ],
        compiler_params=pltpu.CompilerParams(collective_id=0, has_side_effects=True),
        name="gram",
    )(panel.T)
    return c_in + gram.reshape(c_in.shape)


def solution(mesh):
    torus = Mesh(
        mesh.devices.reshape(NX, 2, NY, 2, NL),
        ("x", "zh", "y", "core", "zl"),
    )
    return jax.shard_map(
        on_device,
        mesh=torus,
        in_specs=(
            P("zl", ("y", "core", "x", "zh")),
            P("zl", ("x", "zh"), None, ("y", "core")),
        ),
        out_specs=P("zl", ("x", "zh"), None, ("y", "core")),
        check_vma=False,
    )
```

```python
import functools

import jax
import jax.numpy as jnp
from jax import lax
from jax.experimental import pallas as pl
from jax.experimental.pallas import tpu as pltpu
from jax.sharding import Mesh
from jax.sharding import PartitionSpec as P

NX, NY, NZ, NL = 4, 8, 8, 4
W, DEPTH = 64, 256
C0 = 0
Y0 = 32
D0 = 35
Q0 = 39
P0 = 43
SLOTS = 51
RZ, RX, RY, RD, RQ, DONE, ARRIVALS = 0, 8, 16, 19, 23, 27, 28
LAST_HOPS = 24
DEPARTURES = 4
NEXT, LAST, FAR, SIGNALS = 8, 9, 10, 11

ORDER = (
    (90, 91, 92, 11, 93, 12, 30, 21, 13, 61, 63, 22, 41, 15, 62, 70, 17, 23, 32, 80, 27, 43, 71, 26, 25, 47, 24, 36, 81, 72, 73, 45, 34, 82, 83),
    (90, 91, 92, 12, 93, 13, 41, 20, 22, 61, 63, 14, 30, 23, 32, 17, 62, 71, 43, 70, 24, 81, 80, 72, 27, 34, 73, 26, 25, 82, 83, 47, 36, 45),
    (90, 91, 92, 13, 93, 32, 21, 14, 61, 63, 23, 20, 41, 17, 62, 72, 43, 30, 24, 82, 73, 70, 25, 71, 27, 26, 34, 80, 83, 81, 45, 47, 36),
    (90, 91, 92, 93, 43, 14, 22, 61, 63, 16, 21, 24, 32, 62, 73, 25, 26, 34, 41, 83, 45, 20, 72, 70, 71, 82, 36, 30, 80, 81, 27, 47),
    (90, 91, 92, 15, 93, 16, 34, 23, 17, 61, 63, 25, 22, 43, 62, 70, 26, 45, 32, 27, 21, 36, 80, 71, 47, 72, 41, 20, 81, 73, 82, 30, 83),
    (90, 91, 92, 16, 93, 17, 45, 24, 61, 63, 26, 34, 62, 71, 27, 36, 23, 47, 20, 81, 22, 70, 72, 43, 21, 30, 73, 32, 82, 80, 41, 83),
    (90, 91, 92, 17, 93, 36, 25, 61, 63, 27, 24, 45, 62, 72, 47, 34, 20, 23, 71, 82, 21, 70, 73, 30, 22, 81, 43, 80, 83, 41, 32),
    (90, 91, 92, 93, 47, 20, 26, 61, 63, 25, 21, 62, 73, 22, 30, 36, 24, 45, 72, 41, 71, 83, 70, 32, 23, 81, 82, 80, 34, 43),
)
CROSS = ((7, 5), (7, 4), (7, 4), (4, 6), (3, 1), (0, 3), (0, 3), (0, 2),)
PASS = (
    ((5, (1,)), (6, (1,)), (7, (1,))),
    ((4, (0,)),),
    ((7, (3,)),),
    ((4, (2,)), (5, (2,)), (6, (2,))),
    ((1, (5,)), (2, (5,)), (3, (5,))),
    ((0, (4,)),),
    ((3, (7,)),),
    ((0, (6,)), (1, (6,)), (2, (6,))),
)


def kernel(panel_ref, out_ref, buf, left, acc, send, recv, ready, load):
    x, zh, y = lax.axis_index("x"), lax.axis_index("zh"), lax.axis_index("y")
    core, zl = lax.axis_index("core"), lax.axis_index("zl")
    z = zh * NL + zl
    q = y % 2
    xp, xm = (x + 1) % NX, (x + NX - 1) % NX
    bar = pltpu.get_barrier_semaphore()

    def on_x(t):
        return {"x": t}

    def on_y(d):
        return {"y": (y + NY + d) % NY}

    def on_z(t):
        return {"zh": t // NL, "zl": t % NL}

    other = {"core": 1 - core}

    def signal(sem, where):
        pl.semaphore_signal(sem, inc=1, device_id=where, device_id_type=pl.DeviceIdType.MESH)

    def column_slot(i, t):
        return C0 + t * NX + i

    for where in (on_x(xp), on_x(xm), on_y(1), on_y(-1), other):
        signal(bar, where)
    for t in range(NZ):

        @pl.when(t > z)
        def _():
            signal(bar, on_z(t))

    mine = column_slot(x, z)
    fetch = pltpu.make_async_copy(panel_ref, buf.at[mine], load)
    fetch.start()
    pl.semaphore_wait(bar, 5 + z)
    for t in range(NZ):

        @pl.when(t < z)
        def _():
            signal(ready.at[z], on_z(t))

    signal(ready.at[NEXT], on_y(-1))
    signal(ready.at[LAST], on_y(1))
    fetch.wait()

    def copy(src, dst, to, where, leave=0):
        return pltpu.make_async_remote_copy(
            src_ref=buf.at[src],
            dst_ref=buf.at[dst],
            send_sem=send.at[leave],
            recv_sem=recv.at[to],
            device_id=where,
            device_id_type=pl.DeviceIdType.MESH,
        )

    def arrived(to):
        copy(0, 0, to, other).wait_recv()

    def all_of(count):
        part = buf.at[pl.ds(0, count)]
        return pltpu.make_async_remote_copy(
            src_ref=part,
            dst_ref=part,
            send_sem=send.at[0],
            recv_sem=recv.at[DONE],
            device_id=other,
            device_id_type=pl.DeviceIdType.MESH,
        )

    def z_copy(block, t):
        slot = column_slot(x, block)
        return copy(slot, slot, RZ + block, {"zh": t // NL, "zl": t % NL})

    def x_spread(t):
        slot = column_slot(x, t)
        copy(slot, slot, DONE if t % 2 else RX + t, on_x(xp)).start()
        copy(slot, slot, RX + t if t % 2 else DONE, on_x(xm)).start()

    def x_on(t):
        arrived(RX + t)
        slot = column_slot(xp if t % 2 else xm, t)
        copy(slot, slot, DONE, on_x(xm if t % 2 else xp)).start()

    def y_send(j):
        copy(mine, Y0 + j - 1, RY + j - 1, on_y(2 * j)).start()

    def y_home(j):
        return ((y + NY - 2 * j) % NY) // 2

    def d_copy(j):
        return copy(Y0 + j - 1, D0 + zl, RD + zl, on_z(zh * NL + y_home(j)), j)

    def y_forward(j):
        arrived(RY + j - 1)

        @pl.when(y_home(j) != zl)
        def _():
            d_copy(j).start()

    back = ((y + NY - 2 * zl - q) % NY) // 2

    def row_slot(layer):
        away = jnp.where(zl == layer, Y0 + back - 1, D0 + layer)
        return jnp.where(back == 0, column_slot(x, zh * NL + layer), away)

    def p_copy(slot, parity, layer):
        return copy(slot, P0 + parity * NL + layer, DONE, other)

    def d_forward(layer):
        @pl.when(jnp.logical_and(back != 0, zl != layer))
        def _():
            arrived(RD + layer)

        slot = row_slot(layer)
        copy(slot, Q0 + layer, RQ + layer, on_y(-1 if layer % 2 else 1)).start()
        p_copy(slot, q, layer).start()

    def q_forward(layer):
        arrived(RQ + layer)
        p_copy(Q0 + layer, 1 - q, layer).start()

    def program(place):
        here = place // NL * NL
        near = [t for t in range(here, here + NL) if t != place]
        near.sort(key=lambda t: abs(t - place))
        met = set(range(place + 1))
        count = 3 * NZ + 3 + 12 + len(near) + len(CROSS[place]) + sum(len(to) for _, to in PASS[place])

        def meet(t):
            if t not in met:
                met.add(t)
                pl.semaphore_wait(ready.at[t], 1)

        for t in list(CROSS[place]) + near if here else near:
            if t < place:
                z_copy(place, t).start()
        x_spread(place)
        for code in ORDER[place]:
            step, t = code // 10, code % 10
            if step == 1:
                meet(t)
                z_copy(place, t).start()
            elif step == 2:
                arrived(RZ + t)
                for block, places in PASS[place]:
                    if block == t:
                        for to in places:
                            meet(to)
                            z_copy(block, to).start()
                x_spread(t)
            elif step in (3, 4):
                x_on(t)
            elif step == 6:
                for n in near:
                    meet(n)
                y_forward(t)
            elif step == 7:
                d_forward(t)
            elif step == 8:
                q_forward(t)
            elif t == 0:
                pl.semaphore_wait(ready.at[LAST], 1)
                y_send(3)
            elif t == 1:
                pl.semaphore_wait(ready.at[NEXT], 1)
                y_send(1)
            elif t == 2:
                signal(ready.at[FAR], on_y(-2))
            else:
                pl.semaphore_wait(ready.at[FAR], 1)
                y_send(2)
        for t in range(NZ):
            meet(t)
        all_of(count).wait_send()

    for place in range(NZ):
        pl.when(z == place)(functools.partial(program, place))

    for j in (1, 2, 3):

        @pl.when(y_home(j) != zl)
        def _():
            d_copy(j).wait_send()

    all_of(LAST_HOPS).wait_recv()

    for layer in range(NL):
        for parity in (0, 1):
            own = jnp.where(q == parity, row_slot(layer), Q0 + layer)
            theirs = P0 + parity * NL + layer
            left[pl.ds(parity * 2 * W, W), :] = buf[jnp.where(core == 0, own, theirs)]
            left[pl.ds(parity * 2 * W + W, W), :] = buf[jnp.where(core == 0, theirs, own)]
        for high in (0, 1):
            right = buf[pl.ds(column_slot(0, high * NL + layer), NX)].reshape(NX * W, DEPTH)
            part = lax.dot_general(
                left[...],
                right,
                (((1,), (1,)), ((), ())),
                precision=lax.Precision.HIGHEST,
                preferred_element_type=jnp.float32,
            )
            if layer == 0:
                acc[high] = part
            else:
                acc[high] += part
    first = lax.broadcasted_iota(jnp.int32, (4 * W, 2 * W), 1) < W
    for i in range(NX // 2):
        low, high = (acc[h, :, pl.ds(i * 2 * W, 2 * W)] for h in (0, 1))
        out_ref[:, pl.ds(i * 4 * W, 2 * W)] = jnp.where(first, low, pltpu.roll(high, W, 1))
        out_ref[:, pl.ds(i * 4 * W + 2 * W, 2 * W)] = jnp.where(first, pltpu.roll(low, W, 1), high)


def on_device(panel, c_in):
    gram = pl.pallas_call(
        kernel,
        out_shape=jax.ShapeDtypeStruct((256, 512), jnp.float32),
        in_specs=[pl.BlockSpec(memory_space=pl.ANY)],
        out_specs=pl.BlockSpec(memory_space=pltpu.VMEM),
        scratch_shapes=[
            pltpu.VMEM((SLOTS, W, DEPTH), jnp.float32),
            pltpu.VMEM((4 * W, DEPTH), jnp.float32),
            pltpu.VMEM((2, 4 * W, NX * W), jnp.float32),
            pltpu.SemaphoreType.DMA((DEPARTURES,)),
            pltpu.SemaphoreType.DMA((ARRIVALS,)),
            pltpu.SemaphoreType.REGULAR((SIGNALS,)),
            pltpu.SemaphoreType.DMA,
        ],
        compiler_params=pltpu.CompilerParams(collective_id=0, has_side_effects=True),
        name="gram",
    )(panel.T)
    return c_in + gram.reshape(c_in.shape)


def solution(mesh):
    torus = Mesh(
        mesh.devices.reshape(NX, 2, NY, 2, NL),
        ("x", "zh", "y", "core", "zl"),
    )
    return jax.shard_map(
        on_device,
        mesh=torus,
        in_specs=(
            P("zl", ("y", "core", "x", "zh")),
            P("zl", ("x", "zh"), None, ("y", "core")),
        ),
        out_specs=P("zl", ("x", "zh"), None, ("y", "core")),
        check_vma=False,
    )
```

```python
import functools

import jax
import jax.numpy as jnp
from jax import lax
from jax.experimental import pallas as pl
from jax.experimental.pallas import tpu as pltpu
from jax.sharding import Mesh
from jax.sharding import PartitionSpec as P

NX, NY, NZ, NL = 4, 8, 8, 4
W, DEPTH = 64, 256
C0 = 0
Y0 = 32
D0 = 35
Q0 = 39
P0 = 43
SLOTS = 51
RZ, RX, RY, RD, RQ, DONE, ARRIVALS = 0, 8, 16, 19, 23, 27, 28
LAST_HOPS = 24
DEPARTURES = 4
NEXT, LAST, FAR, ACROSS, SIGNALS = 8, 9, 10, 11, 12

ORDER = (
    (90, 91, 92, 93, 11, 30, 12, 21, 13, 61, 63, 17, 15, 62, 70, 22, 41, 80, 32, 27, 23, 26, 25, 71, 47, 72, 43, 24, 81, 36, 73, 45, 34, 82, 83),
    (90, 91, 92, 12, 93, 13, 41, 20, 22, 61, 63, 14, 17, 30, 23, 32, 62, 71, 70, 43, 24, 81, 80, 72, 27, 34, 26, 25, 73, 82, 47, 36, 45, 83),
    (90, 91, 92, 13, 93, 32, 21, 14, 61, 63, 23, 17, 20, 41, 62, 72, 43, 30, 82, 24, 70, 73, 71, 25, 27, 26, 34, 80, 83, 45, 81, 47, 36),
    (90, 91, 92, 93, 14, 43, 22, 16, 61, 63, 24, 32, 21, 25, 62, 73, 26, 34, 41, 72, 83, 45, 20, 70, 82, 36, 71, 80, 30, 27, 81, 47),
    (90, 91, 92, 15, 16, 93, 17, 34, 23, 25, 61, 63, 22, 43, 26, 62, 70, 45, 27, 21, 32, 80, 71, 36, 72, 81, 20, 47, 41, 73, 82, 30, 83),
    (90, 91, 92, 16, 93, 17, 45, 24, 61, 63, 26, 34, 62, 71, 27, 36, 23, 81, 47, 20, 22, 72, 70, 43, 21, 30, 73, 32, 80, 82, 41, 83),
    (90, 91, 92, 17, 93, 36, 25, 27, 61, 63, 24, 45, 62, 72, 47, 34, 20, 23, 82, 71, 21, 73, 30, 70, 43, 22, 81, 83, 80, 41, 32),
    (90, 91, 92, 93, 47, 20, 61, 63, 26, 21, 25, 30, 62, 73, 22, 36, 41, 24, 45, 72, 83, 71, 23, 82, 70, 32, 81, 34, 43, 80),
)
CROSS = ((7, 5), (7, 4), (7, 4), (4, 6), (3, 1), (0, 3), (0, 3), (0, 2),)
PASS = (
    ((5, (1,)), (6, (1,)), (7, (1,))),
    ((4, (0,)),),
    ((7, (3,)),),
    ((4, (2,)), (5, (2,)), (6, (2,))),
    ((1, (5,)), (2, (5,)), (3, (5,))),
    ((0, (4,)),),
    ((3, (7,)),),
    ((0, (6,)), (1, (6,)), (2, (6,))),
)
PAIR = ((), (), (), (), (), (), (), (),)


def product(left, right):
    def dot(a, b):
        return lax.dot_general(a, b, (((1,), (1,)), ((), ())), preferred_element_type=jnp.float32)

    def terms(value):
        high = value.astype(jnp.bfloat16)
        return high, (value - high.astype(jnp.float32)).astype(jnp.bfloat16)

    (a, c), (b, d) = terms(left), terms(right)
    return dot(a, b) + (dot(a, d) + dot(c, b))


def kernel(panel_ref, out_ref, buf, left, acc, send, recv, ready, load):
    x, zh, y = lax.axis_index("x"), lax.axis_index("zh"), lax.axis_index("y")
    core, zl = lax.axis_index("core"), lax.axis_index("zl")
    z = zh * NL + zl
    q = y % 2
    xp, xm = (x + 1) % NX, (x + NX - 1) % NX
    bar = pltpu.get_barrier_semaphore()

    def on_x(t):
        return {"x": t}

    def on_y(d):
        return {"y": (y + NY + d) % NY}

    def on_z(t):
        return {"zh": t // NL, "zl": t % NL}

    other = {"core": 1 - core}

    def signal(sem, where):
        pl.semaphore_signal(sem, inc=1, device_id=where, device_id_type=pl.DeviceIdType.MESH)

    def column_slot(i, t):
        return C0 + t * NX + i

    for where in (on_x(xp), on_x(xm), on_y(1), on_y(-1), other):
        signal(bar, where)
    for t in range(NZ):

        @pl.when(t > z)
        def _():
            signal(bar, on_z(t))

    mine = column_slot(x, z)
    fetch = pltpu.make_async_copy(panel_ref, buf.at[mine], load)
    fetch.start()
    pl.semaphore_wait(bar, 5 + z)
    for t in range(NZ):

        @pl.when(t < z)
        def _():
            signal(ready.at[z], on_z(t))

    signal(ready.at[NEXT], on_y(-1))
    signal(ready.at[LAST], on_y(1))
    signal(ready.at[ACROSS], on_x(xp))
    fetch.wait()

    def copy(src, dst, to, where, leave=0):
        return pltpu.make_async_remote_copy(
            src_ref=buf.at[src],
            dst_ref=buf.at[dst],
            send_sem=send.at[leave],
            recv_sem=recv.at[to],
            device_id=where,
            device_id_type=pl.DeviceIdType.MESH,
        )

    def arrived(to):
        copy(0, 0, to, other).wait_recv()

    def all_of(count):
        part = buf.at[pl.ds(0, count)]
        return pltpu.make_async_remote_copy(
            src_ref=part,
            dst_ref=part,
            send_sem=send.at[0],
            recv_sem=recv.at[DONE],
            device_id=other,
            device_id_type=pl.DeviceIdType.MESH,
        )

    def z_copy(block, t):
        slot = column_slot(x, block)
        return copy(slot, slot, RZ + block, {"zh": t // NL, "zl": t % NL})

    def x_spread(t, direct):
        slot = column_slot(x, t)
        up, down = (DONE, DONE) if direct else (DONE, RX + t) if t % 2 else (RX + t, DONE)
        copy(slot, slot, up, on_x(xp)).start()
        copy(slot, slot, down, on_x(xm)).start()
        if direct:
            copy(slot, slot, DONE, on_x((x + 2) % NX)).start()

    def x_on(t):
        arrived(RX + t)
        slot = column_slot(xp if t % 2 else xm, t)
        copy(slot, slot, DONE, on_x(xm if t % 2 else xp)).start()

    def y_send(j):
        copy(mine, Y0 + j - 1, RY + j - 1, on_y(2 * j)).start()

    def y_home(j):
        return ((y + NY - 2 * j) % NY) // 2

    def d_copy(j):
        return copy(Y0 + j - 1, D0 + zl, RD + zl, on_z(zh * NL + y_home(j)), j)

    def y_forward(j):
        arrived(RY + j - 1)

        @pl.when(y_home(j) != zl)
        def _():
            d_copy(j).start()

    back = ((y + NY - 2 * zl - q) % NY) // 2

    def row_slot(layer):
        away = jnp.where(zl == layer, Y0 + back - 1, D0 + layer)
        return jnp.where(back == 0, column_slot(x, zh * NL + layer), away)

    def p_copy(slot, parity, layer):
        return copy(slot, P0 + parity * NL + layer, DONE, other)

    def d_forward(layer):
        @pl.when(jnp.logical_and(back != 0, zl != layer))
        def _():
            arrived(RD + layer)

        slot = row_slot(layer)
        copy(slot, Q0 + layer, RQ + layer, on_y(-1 if layer % 2 else 1)).start()
        p_copy(slot, q, layer).start()

    def q_forward(layer):
        arrived(RQ + layer)
        p_copy(Q0 + layer, 1 - q, layer).start()

    def program(place):
        here = place // NL * NL
        near = [t for t in range(here, here + NL) if t != place]
        near.sort(key=lambda t: abs(t - place))
        met = set(range(place + 1))
        count = 3 * NZ + 3 + 12 + len(near) + len(CROSS[place]) + sum(len(to) for _, to in PASS[place])

        def meet(t):
            if t not in met:
                met.add(t)
                pl.semaphore_wait(ready.at[t], 1)

        for t in list(CROSS[place]) + near if here else near:
            if t < place:
                z_copy(place, t).start()
        pair_met = []

        def spread(t):
            if t in PAIR[place] and not pair_met:
                pair_met.append(t)
                pl.semaphore_wait(ready.at[ACROSS], 1)
            x_spread(t, t in PAIR[place])

        spread(place)
        for code in ORDER[place]:
            step, t = code // 10, code % 10
            if step == 1:
                meet(t)
                z_copy(place, t).start()
            elif step == 2:
                arrived(RZ + t)
                for block, places in PASS[place]:
                    if block == t:
                        for to in places:
                            meet(to)
                            z_copy(block, to).start()
                spread(t)
            elif step in (3, 4):
                x_on(t)
            elif step == 6:
                for n in near:
                    meet(n)
                y_forward(t)
            elif step == 7:
                d_forward(t)
            elif step == 8:
                q_forward(t)
            elif t == 0:
                pl.semaphore_wait(ready.at[LAST], 1)
                y_send(3)
            elif t == 1:
                pl.semaphore_wait(ready.at[NEXT], 1)
                y_send(1)
            elif t == 2:
                signal(ready.at[FAR], on_y(-2))
            else:
                pl.semaphore_wait(ready.at[FAR], 1)
                y_send(2)
        for t in range(NZ):
            meet(t)
        if not pair_met:
            pl.semaphore_wait(ready.at[ACROSS], 1)
        all_of(LAST_HOPS + len(PAIR[place])).wait_recv()
        all_of(count).wait_send()

    for place in range(NZ):
        pl.when(z == place)(functools.partial(program, place))

    for j in (1, 2, 3):

        @pl.when(y_home(j) != zl)
        def _():
            d_copy(j).wait_send()

    for layer in range(NL):
        for parity in (0, 1):
            own = jnp.where(q == parity, row_slot(layer), Q0 + layer)
            theirs = P0 + parity * NL + layer
            left[pl.ds(parity * 2 * W, W), :] = buf[jnp.where(core == 0, own, theirs)]
            left[pl.ds(parity * 2 * W + W, W), :] = buf[jnp.where(core == 0, theirs, own)]
        for high in (0, 1):
            right = buf[pl.ds(column_slot(0, high * NL + layer), NX)].reshape(NX * W, DEPTH)
            part = product(left[...], right)
            if layer == 0:
                acc[high] = part
            else:
                acc[high] += part
    first = lax.broadcasted_iota(jnp.int32, (4 * W, 2 * W), 1) < W
    for i in range(NX // 2):
        low, high = (acc[h, :, pl.ds(i * 2 * W, 2 * W)] for h in (0, 1))
        out_ref[:, pl.ds(i * 4 * W, 2 * W)] = jnp.where(first, low, pltpu.roll(high, W, 1))
        out_ref[:, pl.ds(i * 4 * W + 2 * W, 2 * W)] = jnp.where(first, pltpu.roll(low, W, 1), high)


def on_device(panel, c_in):
    gram = pl.pallas_call(
        kernel,
        out_shape=pltpu.VMEM((256, 512), jnp.float32),
        in_specs=[pl.BlockSpec(memory_space=pl.ANY)],
        out_specs=pl.BlockSpec(memory_space=pltpu.VMEM),
        scratch_shapes=[
            pltpu.VMEM((SLOTS, W, DEPTH), jnp.float32),
            pltpu.VMEM((4 * W, DEPTH), jnp.float32),
            pltpu.VMEM((2, 4 * W, NX * W), jnp.float32),
            pltpu.SemaphoreType.DMA((DEPARTURES,)),
            pltpu.SemaphoreType.DMA((ARRIVALS,)),
            pltpu.SemaphoreType.REGULAR((SIGNALS,)),
            pltpu.SemaphoreType.DMA,
        ],
        compiler_params=pltpu.CompilerParams(collective_id=0, has_side_effects=True),
        name="gram",
    )(panel.T)
    return c_in + gram.reshape(c_in.shape)


def solution(mesh):
    torus = Mesh(
        mesh.devices.reshape(NX, 2, NY, 2, NL),
        ("x", "zh", "y", "core", "zl"),
    )
    return jax.shard_map(
        on_device,
        mesh=torus,
        in_specs=(
            P("zl", ("y", "core", "x", "zh")),
            P("zl", ("x", "zh"), None, ("y", "core")),
        ),
        out_specs=P("zl", ("x", "zh"), None, ("y", "core")),
        check_vma=False,
    )
```

```python
import functools

import jax
import jax.numpy as jnp
from jax import lax
from jax.experimental import pallas as pl
from jax.experimental.pallas import tpu as pltpu
from jax.sharding import Mesh
from jax.sharding import PartitionSpec as P

NX, NY, NZ, NL = 4, 8, 8, 4
W, DEPTH = 64, 256
C0 = 0
Y0 = 32
D0 = 35
Q0 = 39
P0 = 43
SLOTS = 51
RZ, RX, RY, RD, RQ, DONE, PAIRED, ARRIVALS = 0, 8, 16, 19, 23, 27, 29, 30
LAST_HOPS = 8
UP, DOWN, FARTHER, DEPARTURES = 2, 4, 5, 6
NEXT, LAST, SIGNALS = 8, 9, 10

ORDER = (
    (90, 91, 11, 30, 12, 21, 13, 61, 63, 70, 17, 15, 80, 22, 41, 50, 27, 32, 71, 23, 26, 25, 72, 47, 81, 73, 24, 43, 36, 51, 82, 45, 83, 52, 34, 53),
    (90, 91, 12, 13, 41, 20, 22, 61, 63, 71, 14, 17, 30, 23, 32, 81, 70, 72, 43, 51, 80, 24, 27, 73, 26, 82, 25, 50, 83, 47, 52, 34, 36, 53, 45),
    (90, 91, 13, 32, 21, 14, 61, 63, 72, 23, 17, 20, 41, 82, 43, 30, 71, 73, 52, 70, 24, 27, 25, 81, 26, 83, 80, 34, 51, 53, 47, 50, 36, 45),
    (90, 91, 14, 43, 22, 16, 61, 63, 73, 24, 25, 32, 21, 83, 72, 26, 34, 53, 71, 82, 45, 20, 41, 70, 81, 27, 36, 52, 80, 30, 51, 47, 50),
    (90, 91, 15, 16, 17, 34, 23, 25, 61, 63, 70, 22, 26, 43, 80, 71, 45, 27, 32, 21, 72, 50, 36, 81, 73, 82, 47, 20, 41, 51, 83, 52, 30, 53),
    (90, 91, 16, 17, 45, 24, 61, 63, 71, 26, 34, 81, 27, 36, 23, 72, 51, 20, 70, 47, 73, 22, 21, 43, 82, 80, 83, 30, 52, 32, 41, 50, 53),
    (90, 91, 17, 36, 25, 27, 63, 61, 72, 24, 45, 71, 47, 82, 34, 20, 23, 52, 70, 73, 81, 21, 22, 80, 30, 83, 43, 51, 53, 41, 32, 50),
    (90, 91, 47, 20, 26, 61, 63, 73, 21, 25, 30, 72, 22, 83, 71, 36, 41, 24, 53, 82, 45, 70, 81, 23, 52, 32, 80, 51, 34, 43, 50),
)
CROSS = ((7, 5), (7, 4), (7, 4), (4, 6), (3, 1), (0, 3), (0, 3), (0, 2),)
PASS = (
    ((5, (1,)), (6, (1,)), (7, (1,))),
    ((4, (0,)),),
    ((7, (3,)),),
    ((4, (2,)), (5, (2,)), (6, (2,))),
    ((1, (5,)), (2, (5,)), (3, (5,))),
    ((0, (4,)),),
    ((3, (7,)),),
    ((0, (6,)), (1, (6,)), (2, (6,))),
)


def product(left, right):
    def dot(a, b):
        return lax.dot_general(a, b, (((1,), (1,)), ((), ())), preferred_element_type=jnp.float32)

    def terms(value):
        high = value.astype(jnp.bfloat16)
        return high, (value - high.astype(jnp.float32)).astype(jnp.bfloat16)

    (a, c), (b, d) = terms(left), terms(right)
    return dot(a, b) + (dot(a, d) + dot(c, b))


def kernel(panel_ref, out_ref, buf, left, acc, send, recv, ready, load):
    x, zh, y = lax.axis_index("x"), lax.axis_index("zh"), lax.axis_index("y")
    core, zl = lax.axis_index("core"), lax.axis_index("zl")
    z = zh * NL + zl
    q = y % 2
    xp, xm = (x + 1) % NX, (x + NX - 1) % NX
    bar = pltpu.get_barrier_semaphore()

    def on_x(t):
        return {"x": t}

    def on_y(d):
        return {"y": (y + NY + d) % NY}

    def on_z(t):
        return {"zh": t // NL, "zl": t % NL}

    other = {"core": 1 - core}

    def signal(sem, where):
        pl.semaphore_signal(sem, inc=1, device_id=where, device_id_type=pl.DeviceIdType.MESH)

    def column_slot(i, t):
        return C0 + t * NX + i

    for where in (on_x(xp), on_x(xm), on_y(1), on_y(-1), other):
        signal(bar, where)
    for t in range(NZ):

        @pl.when(t > z)
        def _():
            signal(bar, on_z(t))

    mine = column_slot(x, z)
    fetch = pltpu.make_async_copy(panel_ref, buf.at[mine], load)
    fetch.start()
    pl.semaphore_wait(bar, 5 + z)
    for t in range(NZ):

        @pl.when(t < z)
        def _():
            signal(ready.at[z], on_z(t))

    signal(ready.at[NEXT], on_y(-1))
    signal(ready.at[LAST], on_y(1))
    fetch.wait()

    def copy(src, dst, to, where, leave=0):
        return pltpu.make_async_remote_copy(
            src_ref=buf.at[src],
            dst_ref=buf.at[dst],
            send_sem=send.at[leave],
            recv_sem=recv.at[to],
            device_id=where,
            device_id_type=pl.DeviceIdType.MESH,
        )

    def arrived(to):
        copy(0, 0, to, other).wait_recv()

    def all_of(count, to=DONE, leave=0):
        part = buf.at[pl.ds(0, count)]
        return pltpu.make_async_remote_copy(
            src_ref=part,
            dst_ref=part,
            send_sem=send.at[leave],
            recv_sem=recv.at[to],
            device_id=other,
            device_id_type=pl.DeviceIdType.MESH,
        )

    def z_copy(block, t):
        slot = column_slot(x, block)
        return copy(slot, slot, RZ + block, {"zh": t // NL, "zl": t % NL})

    def x_spread(t):
        slot, done = column_slot(x, t), DONE + t // NL
        copy(slot, slot, done if t % 2 else RX + t, on_x(xp)).start()
        copy(slot, slot, RX + t if t % 2 else done, on_x(xm)).start()

    def x_on(t):
        arrived(RX + t)
        slot = column_slot(xp if t % 2 else xm, t)
        copy(slot, slot, DONE + t // NL, on_x(xm if t % 2 else xp)).start()

    def y_send(j):
        copy(mine, Y0 + j - 1, RY + j - 1, on_y(2 * j)).start()

    def y_home(j):
        return ((y + NY - 2 * j) % NY) // 2

    def d_copy(j):
        return copy(Y0 + j - 1, D0 + zl, RD + zl, on_z(zh * NL + y_home(j)), j)

    def y_forward(j):
        arrived(RY + j - 1)

        @pl.when(y_home(j) != zl)
        def _():
            d_copy(j).start()

    even = (y + NY - 2 * zl - q) % NY
    back = even // 2
    odd = (even + NY - 1 + 2 * q) % NY

    def row_slot(layer):
        away = jnp.where(jnp.logical_and(zl == layer, back != 2), Y0 + back - 1, D0 + layer)
        return jnp.where(back == 0, column_slot(x, zh * NL + layer), away)

    def p_copy(slot, parity, layer):
        return copy(slot, P0 + parity * NL + layer, PAIRED, other)

    def row_copy(src, dst, to, step, leave):
        return copy(src, dst, to, on_y(step), leave)

    def d_forward(layer):
        @pl.when(back != 2)
        def _():
            @pl.when(jnp.logical_and(back != 0, zl != layer))
            def _():
                arrived(RD + layer)

            slot = row_slot(layer)

            @pl.when(jnp.logical_or(even == 0, even == 2))
            def _():
                row_copy(slot, Q0 + layer, RQ + layer, 1, UP).start()

            @pl.when(jnp.logical_or(even == 0, even == 6))
            def _():
                row_copy(slot, Q0 + layer, RQ + layer, -1, DOWN).start()

            p_copy(slot, q, layer).start()

    def d_far(layer):
        @pl.when(back == 2)
        def _():
            arrived(RD + layer)
            p_copy(D0 + layer, q, layer).start()

    def q_forward(layer):
        arrived(RQ + layer)

        @pl.when(odd == (5 if layer % 2 else 3))
        def _():
            row_copy(Q0 + layer, D0 + layer, RD + layer, -1 if layer % 2 else 1, FARTHER).start()

        p_copy(Q0 + layer, 1 - q, layer).start()

    def program(place):
        here = place // NL * NL
        near = [t for t in range(here, here + NL) if t != place]
        near.sort(key=lambda t: abs(t - place))
        met = set(range(place + 1))
        count = 3 * NZ + 2 + 8 + len(near) + len(CROSS[place]) + sum(len(to) for _, to in PASS[place])

        def meet(t):
            if t not in met:
                met.add(t)
                pl.semaphore_wait(ready.at[t], 1)

        for t in list(CROSS[place]) + near if here else near:
            if t < place:
                z_copy(place, t).start()
        x_spread(place)
        for code in ORDER[place]:
            step, t = code // 10, code % 10
            if step == 1:
                meet(t)
                z_copy(place, t).start()
            elif step == 2:
                arrived(RZ + t)
                for block, places in PASS[place]:
                    if block == t:
                        for to in places:
                            meet(to)
                            z_copy(block, to).start()
                x_spread(t)
            elif step in (3, 4):
                x_on(t)
            elif step == 6:
                for n in near:
                    meet(n)
                y_forward(t)
            elif step == 5:
                d_far(t)
            elif step == 7:
                d_forward(t)
            elif step == 8:
                q_forward(t)
            elif t == 0:
                pl.semaphore_wait(ready.at[LAST], 1)
                y_send(3)
            else:
                pl.semaphore_wait(ready.at[NEXT], 1)
                y_send(1)
        for t in range(NZ):
            meet(t)
        all_of(count).wait_send()

    for place in range(NZ):
        pl.when(z == place)(functools.partial(program, place))

    for j in (1, 3):

        @pl.when(y_home(j) != zl)
        def _():
            d_copy(j).wait_send()

    @pl.when(jnp.logical_or(even == 0, even == 2))
    def _():
        all_of(NL, leave=UP).wait_send()

    @pl.when(jnp.logical_or(even == 0, even == 6))
    def _():
        all_of(NL, leave=DOWN).wait_send()

    @pl.when(jnp.logical_or(odd == 3, odd == 5))
    def _():
        all_of(NL // 2, leave=FARTHER).wait_send()

    all_of(LAST_HOPS, PAIRED).wait_recv()
    for layer in range(NL):
        for parity in (0, 1):
            own = jnp.where(q == parity, row_slot(layer), Q0 + layer)
            theirs = P0 + parity * NL + layer
            left[layer, pl.ds(parity * 2 * W, W), :] = buf[jnp.where(core == 0, own, theirs)]
            left[layer, pl.ds(parity * 2 * W + W, W), :] = buf[jnp.where(core == 0, theirs, own)]
    for half in (zh, 1 - zh):
        all_of(LAST_HOPS, DONE + half).wait_recv()
        for layer in range(NL):
            right = buf[pl.ds(column_slot(0, half * NL + layer), NX)].reshape(NX * W, DEPTH)
            part = product(left[layer], right)
            if layer == 0:
                acc[half] = part
            else:
                acc[half] += part
    first = lax.broadcasted_iota(jnp.int32, (4 * W, 2 * W), 1) < W
    for i in range(NX // 2):
        low, high = (acc[h, :, pl.ds(i * 2 * W, 2 * W)] for h in (0, 1))
        out_ref[:, pl.ds(i * 4 * W, 2 * W)] = jnp.where(first, low, pltpu.roll(high, W, 1))
        out_ref[:, pl.ds(i * 4 * W + 2 * W, 2 * W)] = jnp.where(first, pltpu.roll(low, W, 1), high)


def on_device(panel, c_in):
    gram = pl.pallas_call(
        kernel,
        out_shape=pltpu.VMEM((256, 512), jnp.float32),
        in_specs=[pl.BlockSpec(memory_space=pl.ANY)],
        out_specs=pl.BlockSpec(memory_space=pltpu.VMEM),
        scratch_shapes=[
            pltpu.VMEM((SLOTS, W, DEPTH), jnp.float32),
            pltpu.VMEM((NL, 4 * W, DEPTH), jnp.float32),
            pltpu.VMEM((2, 4 * W, NX * W), jnp.float32),
            pltpu.SemaphoreType.DMA((DEPARTURES,)),
            pltpu.SemaphoreType.DMA((ARRIVALS,)),
            pltpu.SemaphoreType.REGULAR((SIGNALS,)),
            pltpu.SemaphoreType.DMA,
        ],
        compiler_params=pltpu.CompilerParams(collective_id=0, has_side_effects=True),
        name="gram",
    )(panel.T)
    return c_in + gram.reshape(c_in.shape)


def solution(mesh):
    torus = Mesh(
        mesh.devices.reshape(NX, 2, NY, 2, NL),
        ("x", "zh", "y", "core", "zl"),
    )
    return jax.shard_map(
        on_device,
        mesh=torus,
        in_specs=(
            P("zl", ("y", "core", "x", "zh")),
            P("zl", ("x", "zh"), None, ("y", "core")),
        ),
        out_specs=P("zl", ("x", "zh"), None, ("y", "core")),
        check_vma=False,
    )
```

```python
import functools

import jax
import jax.numpy as jnp
from jax import lax
from jax.experimental import pallas as pl
from jax.experimental.pallas import tpu as pltpu
from jax.sharding import Mesh
from jax.sharding import PartitionSpec as P

NX, NY, NZ, NL = 4, 8, 8, 4
W, DEPTH = 64, 256
C0 = 0
Y0 = 32
D0 = 35
Q0 = 39
P0 = 43
SLOTS = 51
RZ, RX, RY, RD, RQ, DONE, PAIRED, ARRIVALS = 0, 8, 16, 19, 23, 27, 29, 30
LAST_HOPS = 8
UP, DOWN, FARTHER, DEPARTURES = 2, 4, 5, 6
NEXT, LAST, SIGNALS = 8, 9, 10

ORDER = (
    (90, 91, 11, 30, 12, 21, 13, 61, 63, 70, 17, 15, 80, 22, 41, 50, 27, 32, 71, 23, 26, 25, 72, 47, 81, 73, 24, 43, 36, 51, 82, 45, 83, 52, 34, 53),
    (90, 91, 12, 13, 41, 20, 22, 61, 63, 71, 14, 17, 30, 23, 32, 81, 70, 72, 43, 51, 80, 24, 27, 73, 26, 82, 25, 50, 83, 47, 52, 34, 36, 53, 45),
    (90, 91, 13, 32, 21, 14, 61, 63, 72, 23, 17, 20, 41, 82, 43, 30, 71, 73, 52, 70, 24, 27, 25, 81, 26, 83, 80, 34, 51, 53, 47, 50, 36, 45),
    (90, 91, 14, 43, 22, 61, 63, 73, 24, 16, 25, 32, 21, 83, 72, 26, 34, 53, 71, 82, 45, 20, 41, 70, 81, 27, 36, 52, 80, 30, 51, 47, 50),
    (90, 91, 15, 16, 17, 34, 23, 25, 61, 63, 70, 22, 26, 43, 80, 71, 45, 27, 32, 21, 72, 50, 36, 81, 73, 82, 47, 20, 41, 51, 83, 52, 30, 53),
    (90, 91, 16, 17, 45, 24, 61, 63, 71, 26, 34, 81, 27, 36, 23, 72, 51, 20, 70, 47, 73, 22, 21, 43, 82, 80, 83, 30, 52, 32, 41, 50, 53),
    (90, 91, 17, 36, 25, 27, 63, 61, 72, 24, 45, 71, 47, 82, 34, 20, 23, 52, 70, 73, 81, 21, 22, 80, 30, 83, 41, 43, 51, 53, 32, 50),
    (90, 91, 47, 20, 26, 61, 63, 73, 21, 25, 30, 72, 22, 83, 71, 36, 41, 24, 53, 82, 45, 70, 81, 23, 52, 32, 80, 51, 34, 43, 50),
)
CROSS = ((7, 5), (7, 4), (7, 4), (4, 6), (3, 1), (0, 3), (0, 3), (0, 2),)
PASS = (
    ((5, (1,)), (6, (1,)), (7, (1,))),
    ((4, (0,)),),
    ((7, (3,)),),
    ((4, (2,)), (5, (2,)), (6, (2,))),
    ((1, (5,)), (2, (5,)), (3, (5,))),
    ((0, (4,)),),
    ((3, (7,)),),
    ((0, (6,)), (1, (6,)), (2, (6,))),
)


def product(left, right):
    def dot(a, b):
        return lax.dot_general(a, b, (((1,), (1,)), ((), ())), preferred_element_type=jnp.float32)

    def terms(value):
        high = value.astype(jnp.bfloat16)
        return high, (value - high.astype(jnp.float32)).astype(jnp.bfloat16)

    (a, c), (b, d) = terms(left), terms(right)
    return dot(a, b) + (dot(a, d) + dot(c, b))


def kernel(panel_ref, out_ref, buf, left, acc, send, recv, ready, load):
    x, zh, y = lax.axis_index("x"), lax.axis_index("zh"), lax.axis_index("y")
    core, zl = lax.axis_index("core"), lax.axis_index("zl")
    z = zh * NL + zl
    q = y % 2
    xp, xm = (x + 1) % NX, (x + NX - 1) % NX
    bar = pltpu.get_barrier_semaphore()

    def on_x(t):
        return {"x": t}

    def on_y(d):
        return {"y": (y + NY + d) % NY}

    def on_z(t):
        return {"zh": t // NL, "zl": t % NL}

    other = {"core": 1 - core}

    def signal(sem, where):
        pl.semaphore_signal(sem, inc=1, device_id=where, device_id_type=pl.DeviceIdType.MESH)

    def column_slot(i, t):
        return C0 + t * NX + i

    for where in (on_x(xp), on_x(xm), on_y(1), on_y(-1), other):
        signal(bar, where)
    for t in range(NZ):

        @pl.when(t > z)
        def _():
            signal(bar, on_z(t))

    mine = column_slot(x, z)
    fetch = pltpu.make_async_copy(panel_ref, buf.at[mine], load)
    fetch.start()
    pl.semaphore_wait(bar, 5 + z)
    for t in range(NZ):

        @pl.when(t < z)
        def _():
            signal(ready.at[z], on_z(t))

    signal(ready.at[NEXT], on_y(-1))
    signal(ready.at[LAST], on_y(1))
    fetch.wait()

    def copy(src, dst, to, where, leave=0):
        return pltpu.make_async_remote_copy(
            src_ref=buf.at[src],
            dst_ref=buf.at[dst],
            send_sem=send.at[leave],
            recv_sem=recv.at[to],
            device_id=where,
            device_id_type=pl.DeviceIdType.MESH,
        )

    def arrived(to):
        copy(0, 0, to, other).wait_recv()

    def all_of(count, to=DONE, leave=0):
        part = buf.at[pl.ds(0, count)]
        return pltpu.make_async_remote_copy(
            src_ref=part,
            dst_ref=part,
            send_sem=send.at[leave],
            recv_sem=recv.at[to],
            device_id=other,
            device_id_type=pl.DeviceIdType.MESH,
        )

    def z_copy(block, t):
        slot = column_slot(x, block)
        return copy(slot, slot, RZ + block, {"zh": t // NL, "zl": t % NL})

    def x_spread(t):
        slot, done = column_slot(x, t), DONE + t // NL
        copy(slot, slot, done if t % 2 else RX + t, on_x(xp)).start()
        copy(slot, slot, RX + t if t % 2 else done, on_x(xm)).start()

    def x_on(t):
        arrived(RX + t)
        slot = column_slot(xp if t % 2 else xm, t)
        copy(slot, slot, DONE + t // NL, on_x(xm if t % 2 else xp)).start()

    def y_send(j):
        copy(mine, Y0 + j - 1, RY + j - 1, on_y(2 * j)).start()

    def y_home(j):
        return ((y + NY - 2 * j) % NY) // 2

    def d_copy(j):
        return copy(Y0 + j - 1, D0 + zl, RD + zl, on_z(zh * NL + y_home(j)), j)

    def y_forward(j):
        arrived(RY + j - 1)

        @pl.when(y_home(j) != zl)
        def _():
            d_copy(j).start()

    even = (y + NY - 2 * zl - q) % NY
    back = even // 2
    odd = (even + NY - 1 + 2 * q) % NY

    def row_slot(layer):
        away = jnp.where(jnp.logical_and(zl == layer, back != 2), Y0 + back - 1, D0 + layer)
        return jnp.where(back == 0, column_slot(x, zh * NL + layer), away)

    def p_copy(slot, parity, layer):
        return copy(slot, P0 + parity * NL + layer, PAIRED, other)

    def row_copy(src, dst, to, step, leave):
        return copy(src, dst, to, on_y(step), leave)

    def d_forward(layer):
        @pl.when(back != 2)
        def _():
            @pl.when(jnp.logical_and(back != 0, zl != layer))
            def _():
                arrived(RD + layer)

            slot = row_slot(layer)

            @pl.when(jnp.logical_or(even == 0, even == 2))
            def _():
                row_copy(slot, Q0 + layer, RQ + layer, 1, UP).start()

            @pl.when(jnp.logical_or(even == 0, even == 6))
            def _():
                row_copy(slot, Q0 + layer, RQ + layer, -1, DOWN).start()

            p_copy(slot, q, layer).start()

    def d_far(layer):
        @pl.when(back == 2)
        def _():
            arrived(RD + layer)
            p_copy(D0 + layer, q, layer).start()

    def q_forward(layer):
        arrived(RQ + layer)

        @pl.when(odd == (5 if layer % 2 else 3))
        def _():
            row_copy(Q0 + layer, D0 + layer, RD + layer, -1 if layer % 2 else 1, FARTHER).start()

        p_copy(Q0 + layer, 1 - q, layer).start()

    def program(place):
        here = place // NL * NL
        near = [t for t in range(here, here + NL) if t != place]
        near.sort(key=lambda t: abs(t - place))
        met = set(range(place + 1))
        count = 3 * NZ + 2 + 8 + len(near) + len(CROSS[place]) + sum(len(to) for _, to in PASS[place])

        def meet(t):
            if t not in met:
                met.add(t)
                pl.semaphore_wait(ready.at[t], 1)

        for t in list(CROSS[place]) + near if here else near:
            if t < place:
                z_copy(place, t).start()
        x_spread(place)
        for code in ORDER[place]:
            step, t = code // 10, code % 10
            if step == 1:
                meet(t)
                z_copy(place, t).start()
            elif step == 2:
                arrived(RZ + t)
                for block, places in PASS[place]:
                    if block == t:
                        for to in places:
                            meet(to)
                            z_copy(block, to).start()
                x_spread(t)
            elif step in (3, 4):
                x_on(t)
            elif step == 6:
                for n in near:
                    meet(n)
                y_forward(t)
            elif step == 5:
                d_far(t)
            elif step == 7:
                d_forward(t)
            elif step == 8:
                q_forward(t)
            elif t == 0:
                pl.semaphore_wait(ready.at[LAST], 1)
                y_send(3)
            else:
                pl.semaphore_wait(ready.at[NEXT], 1)
                y_send(1)
        for t in range(NZ):
            meet(t)
        all_of(count).wait_send()

    for place in range(NZ):
        pl.when(z == place)(functools.partial(program, place))

    for j in (1, 3):

        @pl.when(y_home(j) != zl)
        def _():
            d_copy(j).wait_send()

    @pl.when(jnp.logical_or(even == 0, even == 2))
    def _():
        all_of(NL, leave=UP).wait_send()

    @pl.when(jnp.logical_or(even == 0, even == 6))
    def _():
        all_of(NL, leave=DOWN).wait_send()

    @pl.when(jnp.logical_or(odd == 3, odd == 5))
    def _():
        all_of(NL // 2, leave=FARTHER).wait_send()

    all_of(LAST_HOPS, PAIRED).wait_recv()
    for layer in range(NL):
        for parity in (0, 1):
            own = jnp.where(q == parity, row_slot(layer), Q0 + layer)
            theirs = P0 + parity * NL + layer
            left[layer, pl.ds(parity * 2 * W, W), :] = buf[jnp.where(core == 0, own, theirs)]
            left[layer, pl.ds(parity * 2 * W + W, W), :] = buf[jnp.where(core == 0, theirs, own)]
    for half in (zh, 1 - zh):
        all_of(LAST_HOPS, DONE + half).wait_recv()
        for layer in range(NL):
            right = buf[pl.ds(column_slot(0, half * NL + layer), NX)].reshape(NX * W, DEPTH)
            part = product(left[layer], right)
            if layer == 0:
                acc[half] = part
            else:
                acc[half] += part
    first = lax.broadcasted_iota(jnp.int32, (4 * W, 2 * W), 1) < W
    for i in range(NX // 2):
        low, high = (acc[h, :, pl.ds(i * 2 * W, 2 * W)] for h in (0, 1))
        out_ref[:, pl.ds(i * 4 * W, 2 * W)] = jnp.where(first, low, pltpu.roll(high, W, 1))
        out_ref[:, pl.ds(i * 4 * W + 2 * W, 2 * W)] = jnp.where(first, pltpu.roll(low, W, 1), high)


def on_device(panel, c_in):
    gram = pl.pallas_call(
        kernel,
        out_shape=pltpu.VMEM((256, 512), jnp.float32),
        in_specs=[pl.BlockSpec(memory_space=pl.ANY)],
        out_specs=pl.BlockSpec(memory_space=pltpu.VMEM),
        scratch_shapes=[
            pltpu.VMEM((SLOTS, W, DEPTH), jnp.float32),
            pltpu.VMEM((NL, 4 * W, DEPTH), jnp.float32),
            pltpu.VMEM((2, 4 * W, NX * W), jnp.float32),
            pltpu.SemaphoreType.DMA((DEPARTURES,)),
            pltpu.SemaphoreType.DMA((ARRIVALS,)),
            pltpu.SemaphoreType.REGULAR((SIGNALS,)),
            pltpu.SemaphoreType.DMA,
        ],
        compiler_params=pltpu.CompilerParams(collective_id=0, has_side_effects=True),
        name="gram",
    )(panel.T)
    return c_in + gram.reshape(c_in.shape)


def solution(mesh):
    torus = Mesh(
        mesh.devices.reshape(NX, 2, NY, 2, NL),
        ("x", "zh", "y", "core", "zl"),
    )
    return jax.shard_map(
        on_device,
        mesh=torus,
        in_specs=(
            P("zl", ("y", "core", "x", "zh")),
            P("zl", ("x", "zh"), None, ("y", "core")),
        ),
        out_specs=P("zl", ("x", "zh"), None, ("y", "core")),
        check_vma=False,
    )
```

```python
import functools

import jax
import jax.numpy as jnp
from jax import lax
from jax.experimental import pallas as pl
from jax.experimental.pallas import tpu as pltpu
from jax.sharding import Mesh
from jax.sharding import PartitionSpec as P

NX, NY, NZ, NL = 4, 8, 8, 4
W, DEPTH = 64, 256
C0 = 0
Y0 = 32
D0 = 35
Q0 = 39
P0 = 43
SLOTS = 51
RZ, RX, RY, RD, RQ, DONE, PAIRED, ARRIVALS = 0, 8, 16, 19, 23, 27, 29, 30
LAST_HOPS = 8
UP, DOWN, FARTHER, DEPARTURES = 2, 4, 5, 6
NEXT, LAST, SIGNALS = 8, 9, 10

ORDER = (
    (90, 91, 11, 30, 12, 21, 13, 61, 63, 70, 17, 15, 80, 22, 41, 50, 27, 32, 71, 23, 26, 25, 72, 47, 81, 73, 24, 43, 36, 51, 82, 45, 83, 52, 34, 53),
    (90, 91, 12, 13, 41, 20, 22, 61, 63, 71, 14, 17, 30, 23, 32, 81, 70, 72, 43, 51, 80, 24, 27, 73, 26, 82, 25, 50, 83, 47, 52, 34, 36, 53, 45),
    (90, 91, 13, 32, 21, 14, 61, 63, 72, 23, 17, 20, 41, 82, 43, 30, 71, 73, 52, 70, 24, 27, 25, 81, 26, 83, 80, 34, 51, 53, 47, 50, 36, 45),
    (90, 91, 14, 43, 22, 61, 63, 73, 24, 16, 25, 32, 21, 83, 72, 26, 34, 53, 71, 82, 45, 20, 41, 70, 81, 27, 36, 52, 80, 30, 51, 47, 50),
    (90, 91, 15, 16, 17, 34, 23, 25, 61, 63, 70, 22, 26, 43, 80, 71, 45, 27, 32, 21, 72, 50, 36, 81, 73, 82, 47, 20, 41, 51, 83, 52, 30, 53),
    (90, 91, 16, 17, 45, 24, 61, 63, 71, 26, 34, 81, 27, 36, 23, 72, 51, 20, 70, 47, 73, 22, 21, 43, 82, 80, 83, 30, 52, 32, 41, 50, 53),
    (90, 91, 17, 36, 25, 27, 63, 61, 72, 24, 45, 71, 47, 82, 34, 20, 23, 52, 70, 73, 81, 21, 22, 80, 30, 83, 41, 43, 51, 53, 32, 50),
    (90, 91, 47, 20, 26, 61, 63, 73, 21, 25, 30, 72, 22, 83, 71, 36, 41, 24, 53, 82, 45, 70, 81, 23, 52, 32, 80, 51, 34, 43, 50),
)
CROSS = ((7, 5), (7, 4), (7, 4), (4, 6), (3, 1), (0, 3), (0, 3), (0, 2),)
PASS = (
    ((5, (1,)), (6, (1,)), (7, (1,))),
    ((4, (0,)),),
    ((7, (3,)),),
    ((4, (2,)), (5, (2,)), (6, (2,))),
    ((1, (5,)), (2, (5,)), (3, (5,))),
    ((0, (4,)),),
    ((3, (7,)),),
    ((0, (6,)), (1, (6,)), (2, (6,))),
)


def product(left, right):
    def dot(a, b):
        return lax.dot_general(a, b, (((1,), (1,)), ((), ())), preferred_element_type=jnp.float32)

    def terms(value):
        high = value.astype(jnp.bfloat16)
        return high, (value - high.astype(jnp.float32)).astype(jnp.bfloat16)

    (a, c), (b, d) = terms(left), terms(right)
    return dot(a, b) + (dot(a, d) + dot(c, b))


def kernel(panel_ref, out_ref, buf, left, acc, send, recv, ready, load):
    x, zh, y = lax.axis_index("x"), lax.axis_index("zh"), lax.axis_index("y")
    core, zl = lax.axis_index("core"), lax.axis_index("zl")
    z = zh * NL + zl
    q = y % 2
    xp, xm = (x + 1) % NX, (x + NX - 1) % NX
    bar = pltpu.get_barrier_semaphore()

    def on_x(t):
        return {"x": t}

    def on_y(d):
        return {"y": (y + NY + d) % NY}

    def on_z(t):
        return {"zh": t // NL, "zl": t % NL}

    other = {"core": 1 - core}

    def signal(sem, where):
        pl.semaphore_signal(sem, inc=1, device_id=where, device_id_type=pl.DeviceIdType.MESH)

    def column_slot(i, t):
        return C0 + t * NX + i

    for where in (on_x(xp), on_x(xm), on_y(1), on_y(-1), other):
        signal(bar, where)
    for t in range(NZ):

        @pl.when(t > z)
        def _():
            signal(bar, on_z(t))

    mine = column_slot(x, z)
    fetch = pltpu.make_async_copy(panel_ref, buf.at[mine], load)
    fetch.start()
    pl.semaphore_wait(bar, 5 + z)
    for t in range(NZ):

        @pl.when(t < z)
        def _():
            signal(ready.at[z], on_z(t))

    signal(ready.at[NEXT], on_y(-1))
    signal(ready.at[LAST], on_y(1))
    fetch.wait()

    def copy(src, dst, to, where, leave=0):
        return pltpu.make_async_remote_copy(
            src_ref=buf.at[src],
            dst_ref=buf.at[dst],
            send_sem=send.at[leave],
            recv_sem=recv.at[to],
            device_id=where,
            device_id_type=pl.DeviceIdType.MESH,
        )

    def arrived(to):
        copy(0, 0, to, other).wait_recv()

    def all_of(count, to=DONE, leave=0):
        part = buf.at[pl.ds(0, count)]
        return pltpu.make_async_remote_copy(
            src_ref=part,
            dst_ref=part,
            send_sem=send.at[leave],
            recv_sem=recv.at[to],
            device_id=other,
            device_id_type=pl.DeviceIdType.MESH,
        )

    def z_copy(block, t):
        slot = column_slot(x, block)
        return copy(slot, slot, RZ + block, {"zh": t // NL, "zl": t % NL})

    def x_spread(t):
        slot, done = column_slot(x, t), DONE + t // NL
        copy(slot, slot, done if t % 2 else RX + t, on_x(xp)).start()
        copy(slot, slot, RX + t if t % 2 else done, on_x(xm)).start()

    def x_on(t):
        arrived(RX + t)
        slot = column_slot(xp if t % 2 else xm, t)
        copy(slot, slot, DONE + t // NL, on_x(xm if t % 2 else xp)).start()

    def y_send(j):
        copy(mine, Y0 + j - 1, RY + j - 1, on_y(2 * j)).start()

    def y_home(j):
        return ((y + NY - 2 * j) % NY) // 2

    def d_copy(j):
        return copy(Y0 + j - 1, D0 + zl, RD + zl, on_z(zh * NL + y_home(j)), j)

    def y_forward(j):
        arrived(RY + j - 1)

        @pl.when(y_home(j) != zl)
        def _():
            d_copy(j).start()

    even = (y + NY - 2 * zl - q) % NY
    back = even // 2
    odd = (even + NY - 1 + 2 * q) % NY

    def row_slot(layer):
        away = jnp.where(jnp.logical_and(zl == layer, back != 2), Y0 + back - 1, D0 + layer)
        return jnp.where(back == 0, column_slot(x, zh * NL + layer), away)

    def p_copy(slot, parity, layer):
        return copy(slot, P0 + parity * NL + layer, PAIRED, other)

    def row_copy(src, dst, to, step, leave):
        return copy(src, dst, to, on_y(step), leave)

    def d_forward(layer):
        @pl.when(back != 2)
        def _():
            @pl.when(jnp.logical_and(back != 0, zl != layer))
            def _():
                arrived(RD + layer)

            slot = row_slot(layer)

            @pl.when(jnp.logical_or(even == 0, even == 2))
            def _():
                row_copy(slot, Q0 + layer, RQ + layer, 1, UP).start()

            @pl.when(jnp.logical_or(even == 0, even == 6))
            def _():
                row_copy(slot, Q0 + layer, RQ + layer, -1, DOWN).start()

            p_copy(slot, q, layer).start()

    def d_far(layer):
        @pl.when(back == 2)
        def _():
            arrived(RD + layer)
            p_copy(D0 + layer, q, layer).start()

    def q_forward(layer):
        arrived(RQ + layer)

        @pl.when(odd == (5 if layer % 2 else 3))
        def _():
            row_copy(Q0 + layer, D0 + layer, RD + layer, -1 if layer % 2 else 1, FARTHER).start()

        p_copy(Q0 + layer, 1 - q, layer).start()

    def program(place):
        here = place // NL * NL
        near = [t for t in range(here, here + NL) if t != place]
        near.sort(key=lambda t: abs(t - place))
        met = set(range(place + 1))

        def meet(t):
            if t not in met:
                met.add(t)
                pl.semaphore_wait(ready.at[t], 1)

        for t in list(CROSS[place]) + near if here else near:
            if t < place:
                z_copy(place, t).start()
        x_spread(place)
        for code in ORDER[place]:
            step, t = code // 10, code % 10
            if step == 1:
                meet(t)
                z_copy(place, t).start()
            elif step == 2:
                arrived(RZ + t)
                for block, places in PASS[place]:
                    if block == t:
                        for to in places:
                            meet(to)
                            z_copy(block, to).start()
                x_spread(t)
            elif step in (3, 4):
                x_on(t)
            elif step == 6:
                for n in near:
                    meet(n)
                y_forward(t)
            elif step == 5:
                d_far(t)
            elif step == 7:
                d_forward(t)
            elif step == 8:
                q_forward(t)
            elif t == 0:
                pl.semaphore_wait(ready.at[LAST], 1)
                y_send(3)
            else:
                pl.semaphore_wait(ready.at[NEXT], 1)
                y_send(1)
        for t in range(NZ):
            meet(t)

    for place in range(NZ):
        pl.when(z == place)(functools.partial(program, place))

    all_of(LAST_HOPS, PAIRED).wait_recv()
    for layer in range(NL):
        for parity in (0, 1):
            own = jnp.where(q == parity, row_slot(layer), Q0 + layer)
            theirs = P0 + parity * NL + layer
            left[layer, pl.ds(parity * 2 * W, W), :] = buf[jnp.where(core == 0, own, theirs)]
            left[layer, pl.ds(parity * 2 * W + W, W), :] = buf[jnp.where(core == 0, theirs, own)]
    for half in (zh, 1 - zh):
        all_of(LAST_HOPS, DONE + half).wait_recv()
        for layer in range(NL):
            right = buf[pl.ds(column_slot(0, half * NL + layer), NX)].reshape(NX * W, DEPTH)
            part = product(left[layer], right)
            if layer == 0:
                acc[half] = part
            else:
                acc[half] += part
    first = lax.broadcasted_iota(jnp.int32, (4 * W, 2 * W), 1) < W
    for i in range(NX // 2):
        low, high = (acc[h, :, pl.ds(i * 2 * W, 2 * W)] for h in (0, 1))
        out_ref[:, pl.ds(i * 4 * W, 2 * W)] = jnp.where(first, low, pltpu.roll(high, W, 1))
        out_ref[:, pl.ds(i * 4 * W + 2 * W, 2 * W)] = jnp.where(first, pltpu.roll(low, W, 1), high)

    def departed(place):
        count = 3 * NZ + 2 + 8 + NL - 1 + len(CROSS[place]) + sum(len(to) for _, to in PASS[place])
        all_of(count).wait_send()

    for place in range(NZ):
        pl.when(z == place)(functools.partial(departed, place))

    for j in (1, 3):

        @pl.when(y_home(j) != zl)
        def _():
            d_copy(j).wait_send()

    @pl.when(jnp.logical_or(even == 0, even == 2))
    def _():
        all_of(NL, leave=UP).wait_send()

    @pl.when(jnp.logical_or(even == 0, even == 6))
    def _():
        all_of(NL, leave=DOWN).wait_send()

    @pl.when(jnp.logical_or(odd == 3, odd == 5))
    def _():
        all_of(NL // 2, leave=FARTHER).wait_send()


def on_device(panel, c_in):
    gram = pl.pallas_call(
        kernel,
        out_shape=pltpu.VMEM((256, 512), jnp.float32),
        in_specs=[pl.BlockSpec(memory_space=pl.ANY)],
        out_specs=pl.BlockSpec(memory_space=pltpu.VMEM),
        scratch_shapes=[
            pltpu.VMEM((SLOTS, W, DEPTH), jnp.float32),
            pltpu.VMEM((NL, 4 * W, DEPTH), jnp.float32),
            pltpu.VMEM((2, 4 * W, NX * W), jnp.float32),
            pltpu.SemaphoreType.DMA((DEPARTURES,)),
            pltpu.SemaphoreType.DMA((ARRIVALS,)),
            pltpu.SemaphoreType.REGULAR((SIGNALS,)),
            pltpu.SemaphoreType.DMA,
        ],
        compiler_params=pltpu.CompilerParams(collective_id=0, has_side_effects=True),
        name="gram",
    )(panel.T)
    return c_in + gram.reshape(c_in.shape)


def solution(mesh):
    torus = Mesh(
        mesh.devices.reshape(NX, 2, NY, 2, NL),
        ("x", "zh", "y", "core", "zl"),
    )
    return jax.shard_map(
        on_device,
        mesh=torus,
        in_specs=(
            P("zl", ("y", "core", "x", "zh")),
            P("zl", ("x", "zh"), None, ("y", "core")),
        ),
        out_specs=P("zl", ("x", "zh"), None, ("y", "core")),
        check_vma=False,
    )
```
